32 devices in a mesh: blk: 16 (over z, y, core), head: 2 (over x).
Axes of the slice: x: 2, y: 2, z: 4, core: 2. Of those that a mesh axis runs over, the one named last changes fastest.
Arguments:
- query: bfloat16 [4096, 4096], P(('blk', 'head')), may hold values from -6 to 6
- key: bfloat16 [4096, 1024], P(('blk', 'head')), may hold values from -6 to 6
- value: bfloat16 [4096, 1024], P(('blk', 'head')), may hold values from -6 to 6
- grad_out: bfloat16 [4096, 4096], P(('blk', 'head')), may hold values from -6 to 6
- doc_lengths: int32 [32], replicated, may hold values from 1 to 256, 4096 in all
Outputs:
- attended: bfloat16 [4096, 4096], P(('blk', 'head'))
- grad_query: bfloat16 [4096, 4096], P(('blk', 'head'))
- grad_key: bfloat16 [4096, 1024], P(('blk', 'head'))
- grad_value: bfloat16 [4096, 1024], P(('blk', 'head'))
The draws below stay inside these ranges and needn't reach their ends.
Inputs may be any that keep to these rules, and one draw needn't show every extreme that they name: `doc_lengths`: every document has at most 256 tokens, one has exactly 256, and the lengths sum to 4096.
All inputs are finite; a program needn't handle non-finite values.
Results may differ from the reference program's by a relative error of at most 0.0088.
Values may be sent and summed in bfloat16 or wider, within the bound.
A program may use at most 128 MiB of HBM per device.

```python
import math
import jax
import jax.numpy as jnp
import numpy as np
from jax import lax

HEADS = 32
KV_HEADS = 8
HEAD_DIM = 128
BLOCK = 256
SEQ = 4096
DOC_MOST = 256
DOCS = 32


def draw_query(key, part):
    entry_key = jax.random.fold_in(key, 11)
    result = jnp.clip(jax.random.normal(entry_key, (SEQ, HEADS * HEAD_DIM), jnp.float32), -4.0, 4.0)
    return result.astype(jnp.bfloat16)


def draw_key(key, part):
    entry_key = jax.random.fold_in(key, 12)
    result = jnp.clip(jax.random.normal(entry_key, (SEQ, KV_HEADS * HEAD_DIM), jnp.float32), -4.0, 4.0)
    return result.astype(jnp.bfloat16)


def levels(own_key, dims, shards, low, high):
    factor_of, own = 1.0, jax.random.fold_in(own_key, 6)
    for axis_at, parts in shards:
        heights = jnp.exp(jax.random.uniform(jax.random.fold_in(own, axis_at), (parts,), jnp.float32, low / len(shards), high / len(shards)))
        factor_of = factor_of * jnp.repeat(heights, dims[axis_at] // parts).reshape([-1 if axis == axis_at else 1 for axis in range(len(dims))])
    return factor_of


def split_up(amount, total, limit, lean):
    loads = [(1 << 20) // math.isqrt(rank ** lean) + 1 for rank in range(2, amount + 1)]
    surplus, holding = total - limit - (amount - 1), [1] * (amount - 1)
    while surplus > 0:
        movable = [i for i in range(amount - 1) if holding[i] < limit]
        mass, budget = sum([loads[i] for i in movable]), surplus
        for i in movable:
            extra = min(limit - holding[i], max(1, budget * loads[i] // mass), surplus)
            holding[i] = holding[i] + extra
            surplus = surplus - extra
    return np.array([limit] + holding)


def uneven_parts(stream_key, amount, total, reach, lean):
    if amount == 2:
        one = jax.random.randint(stream_key, (), max(1, total - reach), min(reach, total - 1) + 1)
        return jnp.stack([one, total - one])
    tallies = jnp.asarray(split_up(amount, total, reach, lean), jnp.int32)
    couples = (amount - 1) // 2
    source_of, sink = tallies[1:1 + 2 * couples:2], tallies[2:2 + 2 * couples:2]
    margin = jnp.minimum(source_of - 1, reach - sink)
    moved = jax.random.randint(jax.random.fold_in(stream_key, 1), (couples,), 0, 1 << 20) % (margin + 1)
    tallies = tallies.at[1:1 + 2 * couples:2].set(source_of - moved).at[2:2 + 2 * couples:2].set(sink + moved)
    return tallies[jax.random.permutation(jax.random.fold_in(stream_key, 2), amount)]


def gaussian(key, extent, scale, most, split=(), kind=jnp.bfloat16):
    loudness = levels(key, extent, split, -0.22, 0.18) if split else 1.0
    values = jax.random.normal(key, extent, jnp.float32) * scale * loudness
    return jnp.minimum(jnp.maximum(values, -most), most).astype(kind)


def setup_inputs(seed: int = 0) -> dict:
    keys = jax.random.split(jax.random.key(seed), 6)
    query = draw_query(jax.random.fold_in(keys[5], 71), 0)
    key = draw_key(jax.random.fold_in(keys[5], 71), 0)
    value = gaussian(keys[2], (SEQ, KV_HEADS * HEAD_DIM), 1.0, 6.0, ((0, 32),))
    grad_out = gaussian(keys[3], (SEQ, HEADS * HEAD_DIM), 1.0, 6.0, ((0, 32),))
    doc_lengths = uneven_parts(keys[4], DOCS, SEQ, DOC_MOST, 2).astype(jnp.int32)
    return {"query": query, "key": key, "value": value, "grad_out": grad_out, "doc_lengths": doc_lengths}


def segment_ids(positions, doc_starts):
    return jnp.sum((doc_starts[None, :] <= positions[:, None]).astype(jnp.int32), axis=1) - 1


def reference(query, key, value, grad_out, doc_lengths):
    scaling = HEAD_DIM ** -0.5
    groups = HEADS // KV_HEADS
    row_step = min(512, BLOCK)
    span_rows = DOC_MOST + row_step
    doc_ends = jnp.cumsum(doc_lengths).astype(jnp.int32)
    doc_starts = (doc_ends - doc_lengths).astype(jnp.int32)
    padding = jnp.zeros((DOC_MOST, KV_HEADS * HEAD_DIM), key.dtype)
    keys_padded = jnp.concatenate([padding, key], axis=0)
    values_padded = jnp.concatenate([padding, value], axis=0)
    offsets = jnp.arange(row_step, dtype=jnp.int32)
    reaches = jnp.arange(span_rows, dtype=jnp.int32)

    def visit(carry, tile_number):
        grad_keys, grad_values = carry
        first_row = (tile_number * row_step).astype(jnp.int32)
        query_rows = lax.dynamic_slice_in_dim(query, first_row, row_step, 0).astype(jnp.float32).reshape(row_step, KV_HEADS, groups, HEAD_DIM)
        grad_rows = lax.dynamic_slice_in_dim(grad_out, first_row, row_step, 0).astype(jnp.float32).reshape(row_step, KV_HEADS, groups, HEAD_DIM)
        key_rows = lax.dynamic_slice_in_dim(keys_padded, first_row, span_rows, 0).astype(jnp.float32).reshape(span_rows, KV_HEADS, HEAD_DIM)
        value_rows = lax.dynamic_slice_in_dim(values_padded, first_row, span_rows, 0).astype(jnp.float32).reshape(span_rows, KV_HEADS, HEAD_DIM)
        query_pos = first_row + offsets
        key_pos = first_row - DOC_MOST + reaches
        allowed = (key_pos[None, :] <= query_pos[:, None]) & (segment_ids(query_pos, doc_starts)[:, None] == segment_ids(key_pos, doc_starts)[None, :])
        scores = jnp.einsum('qkgd,skd->kgqs', query_rows, key_rows) * scaling
        scores = jnp.where(allowed[None, None], scores, -jnp.inf)
        peak_score = jnp.max(scores, axis=-1, keepdims=True)
        log_total = peak_score + jnp.log(jnp.sum(jnp.exp(scores - peak_score), axis=-1, keepdims=True))
        weights = jnp.exp(scores - log_total)
        weights_bf = lax.optimization_barrier(weights.astype(jnp.bfloat16)).astype(jnp.float32)
        attended_rows = jnp.einsum('kgqs,skd->qkgd', weights_bf, value_rows).astype(jnp.bfloat16)
        output_rows = lax.optimization_barrier(attended_rows).astype(jnp.float32)
        row_delta = jnp.einsum('qkgd,qkgd->kgq', grad_rows, output_rows)
        grad_weights = jnp.einsum('qkgd,skd->kgqs', grad_rows, value_rows)
        grad_scores = weights * (grad_weights - row_delta[..., None])
        grad_scores = lax.optimization_barrier(grad_scores.astype(jnp.bfloat16)).astype(jnp.float32)
        grad_query_rows = (jnp.einsum('kgqs,skd->qkgd', grad_scores, key_rows) * scaling).astype(jnp.bfloat16)
        key_part = (jnp.einsum('kgqs,qkgd->skd', grad_scores, query_rows) * scaling).reshape(span_rows, KV_HEADS * HEAD_DIM)
        value_part = jnp.einsum('kgqs,qkgd->skd', weights_bf, grad_rows).reshape(span_rows, KV_HEADS * HEAD_DIM)
        current_keys = lax.dynamic_slice_in_dim(grad_keys, first_row, span_rows, 0)
        current_values = lax.dynamic_slice_in_dim(grad_values, first_row, span_rows, 0)
        grad_keys = lax.dynamic_update_slice_in_dim(grad_keys, current_keys + key_part, first_row, 0)
        grad_values = lax.dynamic_update_slice_in_dim(grad_values, current_values + value_part, first_row, 0)
        outputs = (attended_rows.reshape(row_step, HEADS * HEAD_DIM), grad_query_rows.reshape(row_step, HEADS * HEAD_DIM))
        return (grad_keys, grad_values), outputs

    start_keys = jnp.zeros((SEQ + DOC_MOST, KV_HEADS * HEAD_DIM), jnp.float32)
    start_values = jnp.zeros((SEQ + DOC_MOST, KV_HEADS * HEAD_DIM), jnp.float32)
    tile_numbers = jnp.arange(SEQ // row_step, dtype=jnp.int32)
    sums, stacked = lax.scan(visit, (start_keys, start_values), tile_numbers)
    attended = stacked[0].reshape(SEQ, HEADS * HEAD_DIM)
    grad_query = stacked[1].reshape(SEQ, HEADS * HEAD_DIM)
    grad_key = sums[0][DOC_MOST:].astype(jnp.bfloat16)
    grad_value = sums[1][DOC_MOST:].astype(jnp.bfloat16)
    return (attended, grad_query, grad_key, grad_value)
```

```python
import functools
import math

import jax
import jax.numpy as jnp
from jax import lax
from jax.experimental import pallas as pl
from jax.experimental.pallas import tpu as pltpu
from jax.sharding import PartitionSpec as P

HEAD_DIM = 128
EXCLUDED = -1e30
MESH = pl.DeviceIdType.MESH


def kernel(
    back, total, lens, q_hbm, k_hbm, v_hbm, do_hbm, att_hbm, dq_hbm, dk_hbm, dv_hbm,
    window, qbuf, dobuf, attbuf, dqbuf, part, landed, own, summed, bias,
    kv_in, q_in, out_sem, sum_sem, kv_send, kv_recv, g_send, g_recv,
):
    rows = q_hbm.shape[0]
    kv_heads = k_hbm.shape[1] // HEAD_DIM
    groups = q_hbm.shape[1] // k_hbm.shape[1]
    width = groups * HEAD_DIM
    span = (back + 1) * rows
    scaling = HEAD_DIM ** (-0.5)
    me = lax.axis_index("blk") * back + lax.axis_index("head")

    def device(number):
        return {"blk": number // back, "head": number % back}

    def columns(g, size):
        return pl.ds(pl.multiple_of(g * size, size), size)

    def slot(k):
        return pl.ds((back - k) * rows, rows)

    def kv_load(g, which):
        return pltpu.make_async_copy(
            (k_hbm, v_hbm)[which].at[:, columns(g, HEAD_DIM)],
            window.at[g, which, slot(0), :],
            kv_in.at[which, g],
        )

    def q_load(g, which):
        return pltpu.make_async_copy(
            (q_hbm, do_hbm)[which].at[:, columns(g, width)],
            (qbuf, dobuf)[which].at[g],
            q_in.at[which, g],
        )

    def result(g, which):
        return pltpu.make_async_copy(
            (attbuf, dqbuf)[which].at[g],
            (att_hbm, dq_hbm)[which].at[:, columns(g, width)],
            out_sem.at[which, g],
        )

    def sum_result(g, which):
        return pltpu.make_async_copy(
            summed.at[g, which],
            (dk_hbm, dv_hbm)[which].at[:, columns(g, HEAD_DIM)],
            sum_sem.at[which, g],
        )

    def kv_copy(g, k):
        return pltpu.make_async_remote_copy(
            src_ref=window.at[g, :, slot(0), :],
            dst_ref=window.at[g, :, slot(k), :],
            send_sem=kv_send.at[k - 1, g],
            recv_sem=kv_recv.at[k - 1, g],
            device_id=device(me + k),
            device_id_type=MESH,
        )

    def g_copy(g, k):
        return pltpu.make_async_remote_copy(
            src_ref=part.at[g, :, slot(k), :],
            dst_ref=landed.at[g, k - 1],
            send_sem=g_send.at[k - 1, g],
            recv_sem=g_recv.at[k - 1, g],
            device_id=device(me - k),
            device_id_type=MESH,
        )

    @pl.loop(0, kv_heads)
    def _(g):
        kv_load(g, 0).start()
        kv_load(g, 1).start()

    barrier = pltpu.get_barrier_semaphore()
    for k in range(1, back + 1):
        @pl.when(me + k < total)
        def _():
            pl.semaphore_signal(barrier, inc=1, device_id=device(me + k), device_id_type=MESH)

        @pl.when(me - k >= 0)
        def _():
            pl.semaphore_signal(barrier, inc=1, device_id=device(me - k), device_id_type=MESH)

    @pl.loop(0, kv_heads)
    def _(g):
        q_load(g, 0).start()
        q_load(g, 1).start()

    greeted = jnp.minimum(me, back) + jnp.minimum(total - 1 - me, back)
    pl.semaphore_wait(barrier, greeted)

    @pl.loop(0, kv_heads)
    def _(g):
        kv_load(g, 0).wait()
        kv_load(g, 1).wait()
        for k in range(1, back + 1):
            @pl.when(me + k < total)
            def _():
                kv_copy(g, k).start()

    for k in range(1, back + 1):
        @pl.when(me - k < 0)
        def _():
            window[:, :, slot(k), :] = jnp.zeros((kv_heads, 2, rows, HEAD_DIM), jnp.bfloat16)

        @pl.when(me + k >= total)
        def _():
            landed[:, k - 1] = jnp.zeros((kv_heads, 2, rows, HEAD_DIM), jnp.bfloat16)

    query_pos = me * rows + lax.broadcasted_iota(jnp.int32, (1, rows), 1)

    def latest(d, carry):
        start, first = carry
        return start + lens[d], jnp.where(query_pos >= start, start, first)

    _, first = lax.fori_loop(
        0, lens.shape[0], latest, (jnp.int32(0), jnp.zeros((1, rows), jnp.int32))
    )
    key_pos = (me - back) * rows + lax.broadcasted_iota(jnp.int32, (span, rows), 0)
    bias[...] = jnp.where((key_pos <= query_pos) & (key_pos >= first), 0.0, EXCLUDED)

    def dot(a, b, a_dim, b_dim):
        return lax.dot_general(
            a, b, (((a_dim,), (b_dim,)), ((), ())), preferred_element_type=jnp.float32
        )

    def stacked(values):
        return jnp.concatenate(
            [values[:, h * HEAD_DIM : (h + 1) * HEAD_DIM] for h in range(groups)], axis=0
        )

    @pl.loop(0, kv_heads)
    def _(g):
        q_load(g, 0).wait()
        q_load(g, 1).wait()
        for k in range(1, back + 1):
            @pl.when(me - k >= 0)
            def _():
                kv_copy(g, k).wait_recv()

        keys, values = window[g, 0], window[g, 1]
        queries, grads = stacked(qbuf[g]), stacked(dobuf[g])
        kept = jnp.concatenate([bias[...]] * groups, axis=1)
        scores = dot(keys, queries, 1, 1) * (scaling * math.log2(math.e)) + kept
        peak = jnp.max(scores, axis=0, keepdims=True)
        raised = jnp.exp2(scores - peak)
        weights = raised * (1.0 / jnp.sum(raised, axis=0, keepdims=True))
        weights_bf = weights.astype(jnp.bfloat16)
        attended = dot(values, weights_bf, 0, 0)
        grad_weights = dot(values, grads, 1, 1)
        delta = jnp.sum(weights * grad_weights, axis=0, keepdims=True)
        grad_scores = (weights * (grad_weights - delta)).astype(jnp.bfloat16)
        grad_query = dot(keys, grad_scores, 0, 0) * scaling
        grad_key = dot(grad_scores, queries, 1, 0) * scaling
        grad_value = dot(weights_bf, grads, 1, 0)
        part[g, 0] = grad_key[: back * rows].astype(jnp.bfloat16)
        part[g, 1] = grad_value[: back * rows].astype(jnp.bfloat16)
        own[g, 0] = grad_key[back * rows :]
        own[g, 1] = grad_value[back * rows :]
        for h in range(groups):
            at = slice(h * HEAD_DIM, (h + 1) * HEAD_DIM)
            attbuf[g, :, at] = attended[:, at].T.astype(jnp.bfloat16)
            dqbuf[g, :, at] = grad_query[:, at].T.astype(jnp.bfloat16)
        for k in range(1, back + 1):
            @pl.when(me - k >= 0)
            def _():
                g_copy(g, k).start()
        result(g, 0).start()
        result(g, 1).start()

    @pl.loop(0, kv_heads)
    def _(g):
        for k in range(1, back + 1):
            @pl.when(me + k < total)
            def _():
                g_copy(g, k).wait_recv()
        sums = own[g]
        for k in range(1, back + 1):
            sums = sums + landed[g, k - 1].astype(jnp.float32)
        summed[g] = sums.astype(jnp.bfloat16)
        sum_result(g, 0).start()
        sum_result(g, 1).start()

    @pl.loop(0, kv_heads)
    def _(g):
        for k in range(1, back + 1):
            @pl.when(me + k < total)
            def _():
                kv_copy(g, k).wait_send()

            @pl.when(me - k >= 0)
            def _():
                g_copy(g, k).wait_send()
        for which in range(2):
            result(g, which).wait()
            sum_result(g, which).wait()


def solution(mesh):
    back = mesh.shape["head"]
    total = mesh.shape["blk"] * back

    def per_device(query, key, value, grad_out, doc_lengths):
        rows, kv_heads = query.shape[0], key.shape[1] // HEAD_DIM
        width = query.shape[1] // kv_heads
        bf, f32 = jnp.bfloat16, jnp.float32
        anywhere = pl.BlockSpec(memory_space=pl.ANY)
        dma = pltpu.SemaphoreType.DMA
        return pl.pallas_call(
            functools.partial(kernel, back, total),
            out_shape=[
                jax.ShapeDtypeStruct(query.shape, bf),
                jax.ShapeDtypeStruct(query.shape, bf),
                jax.ShapeDtypeStruct(key.shape, bf),
                jax.ShapeDtypeStruct(key.shape, bf),
            ],
            in_specs=[pl.BlockSpec(memory_space=pltpu.SMEM)] + [anywhere] * 4,
            out_specs=[anywhere] * 4,
            scratch_shapes=[
                pltpu.VMEM((kv_heads, 2, (back + 1) * rows, HEAD_DIM), bf),
                pltpu.VMEM((kv_heads, rows, width), bf),
                pltpu.VMEM((kv_heads, rows, width), bf),
                pltpu.VMEM((kv_heads, rows, width), bf),
                pltpu.VMEM((kv_heads, rows, width), bf),
                pltpu.VMEM((kv_heads, 2, back * rows, HEAD_DIM), bf),
                pltpu.VMEM((kv_heads, back, 2, rows, HEAD_DIM), bf),
                pltpu.VMEM((kv_heads, 2, rows, HEAD_DIM), f32),
                pltpu.VMEM((kv_heads, 2, rows, HEAD_DIM), bf),
                pltpu.VMEM(((back + 1) * rows, rows), f32),
                dma((2, kv_heads)),
                dma((2, kv_heads)),
                dma((2, kv_heads)),
                dma((2, kv_heads)),
                dma((back, kv_heads)),
                dma((back, kv_heads)),
                dma((back, kv_heads)),
                dma((back, kv_heads)),
            ],
            compiler_params=pltpu.CompilerParams(collective_id=0, has_side_effects=True),
        )(doc_lengths, query, key, value, grad_out)

    split = P(("blk", "head"), None)
    return jax.shard_map(
        per_device,
        mesh=mesh,
        in_specs=(split, split, split, split, P()),
        out_specs=(split, split, split, split),
        check_vma=False,
    )
```

```python
import functools
import math

import jax
import jax.numpy as jnp
from jax import lax
from jax.experimental import pallas as pl
from jax.experimental.pallas import tpu as pltpu
from jax.sharding import PartitionSpec as P

HEAD_DIM = 128
EXCLUDED = -1e30
MESH = pl.DeviceIdType.MESH


def kernel(
    back, total, lens, q_hbm, k_hbm, v_hbm, do_hbm, attbuf, dqbuf, summed,
    window, qbuf, dobuf, part, landed, own, bias,
    kv_in, q_in, kv_send, kv_recv, g_send, g_recv,
):
    rows = q_hbm.shape[0]
    kv_heads = k_hbm.shape[1] // HEAD_DIM
    groups = q_hbm.shape[1] // k_hbm.shape[1]
    width = groups * HEAD_DIM
    span = (back + 1) * rows
    scaling = HEAD_DIM ** (-0.5)
    me = lax.axis_index("blk") * back + lax.axis_index("head")

    def device(number):
        return {"blk": number // back, "head": number % back}

    def columns(g, size):
        return pl.ds(pl.multiple_of(g * size, size), size)

    def slot(k):
        return pl.ds((back - k) * rows, rows)

    def kv_load(g, which):
        return pltpu.make_async_copy(
            (k_hbm, v_hbm)[which].at[:, columns(g, HEAD_DIM)],
            window.at[g, which, slot(0), :],
            kv_in.at[which, g],
        )

    def q_load(g, which):
        return pltpu.make_async_copy(
            (q_hbm, do_hbm)[which].at[:, columns(g, width)],
            (qbuf, dobuf)[which].at[g],
            q_in.at[which, g],
        )

    def kv_copy(g, k):
        return pltpu.make_async_remote_copy(
            src_ref=window.at[g, :, slot(0), :],
            dst_ref=window.at[g, :, slot(k), :],
            send_sem=kv_send.at[k - 1, g],
            recv_sem=kv_recv.at[k - 1, g],
            device_id=device(me + k),
            device_id_type=MESH,
        )

    def g_copy(g, k):
        return pltpu.make_async_remote_copy(
            src_ref=part.at[g, :, slot(k), :],
            dst_ref=landed.at[g, k - 1],
            send_sem=g_send.at[k - 1, g],
            recv_sem=g_recv.at[k - 1, g],
            device_id=device(me - k),
            device_id_type=MESH,
        )

    @pl.loop(0, kv_heads)
    def _(g):
        kv_load(g, 0).start()
        kv_load(g, 1).start()

    barrier = pltpu.get_barrier_semaphore()
    for k in range(1, back + 1):
        @pl.when(me + k < total)
        def _():
            pl.semaphore_signal(barrier, inc=1, device_id=device(me + k), device_id_type=MESH)

        @pl.when(me - k >= 0)
        def _():
            pl.semaphore_signal(barrier, inc=1, device_id=device(me - k), device_id_type=MESH)

    @pl.loop(0, kv_heads)
    def _(g):
        q_load(g, 0).start()
        q_load(g, 1).start()

    greeted = jnp.minimum(me, back) + jnp.minimum(total - 1 - me, back)
    pl.semaphore_wait(barrier, greeted)

    @pl.loop(0, kv_heads)
    def _(g):
        kv_load(g, 0).wait()
        kv_load(g, 1).wait()
        for k in range(1, back + 1):
            @pl.when(me + k < total)
            def _():
                kv_copy(g, k).start()

    for k in range(1, back + 1):
        @pl.when(me - k < 0)
        def _():
            window[:, :, slot(k), :] = jnp.zeros((kv_heads, 2, rows, HEAD_DIM), jnp.bfloat16)

        @pl.when(me + k >= total)
        def _():
            landed[:, k - 1] = jnp.zeros((kv_heads, 2, rows, HEAD_DIM), jnp.bfloat16)

    query_pos = me * rows + lax.broadcasted_iota(jnp.int32, (1, rows), 1)

    def latest(d, carry):
        start, first = carry
        return start + lens[d], jnp.where(query_pos >= start, start, first)

    _, first = lax.fori_loop(
        0, lens.shape[0], latest, (jnp.int32(0), jnp.zeros((1, rows), jnp.int32))
    )
    key_pos = (me - back) * rows + lax.broadcasted_iota(jnp.int32, (span, rows), 0)
    bias[...] = jnp.where((key_pos <= query_pos) & (key_pos >= first), 0.0, EXCLUDED)

    def dot(a, b, a_dim, b_dim):
        return lax.dot_general(
            a, b, (((a_dim,), (b_dim,)), ((), ())), preferred_element_type=jnp.float32
        )

    def stacked(values):
        return jnp.concatenate(
            [values[:, h * HEAD_DIM : (h + 1) * HEAD_DIM] for h in range(groups)], axis=0
        )

    @pl.loop(0, kv_heads)
    def _(g):
        q_load(g, 0).wait()
        q_load(g, 1).wait()
        for k in range(1, back + 1):
            @pl.when(me - k >= 0)
            def _():
                kv_copy(g, k).wait_recv()

        keys, values = window[g, 0], window[g, 1]
        queries, grads = stacked(qbuf[g]), stacked(dobuf[g])
        kept = jnp.concatenate([bias[...]] * groups, axis=1)
        scores = dot(keys, queries, 1, 1) * (scaling * math.log2(math.e)) + kept
        peak = jnp.max(scores, axis=0, keepdims=True)
        raised = jnp.exp2(scores - peak)
        weights = raised * (1.0 / jnp.sum(raised, axis=0, keepdims=True))
        weights_bf = weights.astype(jnp.bfloat16)
        attended = dot(values, weights_bf, 0, 0)
        grad_weights = dot(values, grads, 1, 1)
        delta = jnp.sum(weights * grad_weights, axis=0, keepdims=True)
        grad_scores = (weights * (grad_weights - delta)).astype(jnp.bfloat16)
        grad_query = dot(keys, grad_scores, 0, 0) * scaling
        grad_key = dot(grad_scores, queries, 1, 0) * scaling
        grad_value = dot(weights_bf, grads, 1, 0)
        part[g, 0] = grad_key[: back * rows].astype(jnp.bfloat16)
        part[g, 1] = grad_value[: back * rows].astype(jnp.bfloat16)
        own[g, 0] = grad_key[back * rows :]
        own[g, 1] = grad_value[back * rows :]
        for h in range(groups):
            at = slice(h * HEAD_DIM, (h + 1) * HEAD_DIM)
            attbuf[g, :, at] = attended[:, at].T.astype(jnp.bfloat16)
            dqbuf[g, :, at] = grad_query[:, at].T.astype(jnp.bfloat16)
        for k in range(1, back + 1):
            @pl.when(me - k >= 0)
            def _():
                g_copy(g, k).start()

    @pl.loop(0, kv_heads)
    def _(g):
        for k in range(1, back + 1):
            @pl.when(me + k < total)
            def _():
                g_copy(g, k).wait_recv()
        sums = own[g]
        for k in range(1, back + 1):
            sums = sums + landed[g, k - 1].astype(jnp.float32)
        summed[g] = sums.astype(jnp.bfloat16)

    @pl.loop(0, kv_heads)
    def _(g):
        for k in range(1, back + 1):
            @pl.when(me + k < total)
            def _():
                kv_copy(g, k).wait_send()

            @pl.when(me - k >= 0)
            def _():
                g_copy(g, k).wait_send()


def write_out(attbuf, dqbuf, summed, att_hbm, dq_hbm, dk_hbm, dv_hbm, sems):
    kv_heads, width = attbuf.shape[0], attbuf.shape[2]
    copies = []
    for g in range(kv_heads):
        wide = slice(g * width, (g + 1) * width)
        narrow = slice(g * HEAD_DIM, (g + 1) * HEAD_DIM)
        for which, (source, target) in enumerate((
            (attbuf.at[g], att_hbm.at[:, wide]),
            (dqbuf.at[g], dq_hbm.at[:, wide]),
            (summed.at[g, 0], dk_hbm.at[:, narrow]),
            (summed.at[g, 1], dv_hbm.at[:, narrow]),
        )):
            copies.append(pltpu.make_async_copy(source, target, sems.at[which, g]))
    for copy in copies:
        copy.start()
    for copy in copies:
        copy.wait()


def solution(mesh):
    back = mesh.shape["head"]
    total = mesh.shape["blk"] * back

    def per_device(query, key, value, grad_out, doc_lengths):
        rows, kv_heads = query.shape[0], key.shape[1] // HEAD_DIM
        width = query.shape[1] // kv_heads
        bf, f32 = jnp.bfloat16, jnp.float32
        anywhere = pl.BlockSpec(memory_space=pl.ANY)
        dma = pltpu.SemaphoreType.DMA
        results = pl.pallas_call(
            functools.partial(kernel, back, total),
            out_shape=[
                pltpu.VMEM((kv_heads, rows, width), bf),
                pltpu.VMEM((kv_heads, rows, width), bf),
                pltpu.VMEM((kv_heads, 2, rows, HEAD_DIM), bf),
            ],
            in_specs=[pl.BlockSpec(memory_space=pltpu.SMEM)] + [anywhere] * 4,
            out_specs=[pl.BlockSpec(memory_space=pltpu.VMEM)] * 3,
            scratch_shapes=[
                pltpu.VMEM((kv_heads, 2, (back + 1) * rows, HEAD_DIM), bf),
                pltpu.VMEM((kv_heads, rows, width), bf),
                pltpu.VMEM((kv_heads, rows, width), bf),
                pltpu.VMEM((kv_heads, 2, back * rows, HEAD_DIM), bf),
                pltpu.VMEM((kv_heads, back, 2, rows, HEAD_DIM), bf),
                pltpu.VMEM((kv_heads, 2, rows, HEAD_DIM), f32),
                pltpu.VMEM(((back + 1) * rows, rows), f32),
                dma((2, kv_heads)),
                dma((2, kv_heads)),
                dma((back, kv_heads)),
                dma((back, kv_heads)),
                dma((back, kv_heads)),
                dma((back, kv_heads)),
            ],
            compiler_params=pltpu.CompilerParams(collective_id=0, has_side_effects=True),
        )(doc_lengths, query, key, value, grad_out)
        results = [pltpu.with_memory_space_constraint(r, pltpu.VMEM) for r in results]
        return pl.pallas_call(
            write_out,
            out_shape=[
                jax.ShapeDtypeStruct(query.shape, bf),
                jax.ShapeDtypeStruct(query.shape, bf),
                jax.ShapeDtypeStruct(key.shape, bf),
                jax.ShapeDtypeStruct(key.shape, bf),
            ],
            in_specs=[pl.BlockSpec(memory_space=pltpu.VMEM)] * 3,
            out_specs=[anywhere] * 4,
            scratch_shapes=[dma((4, kv_heads))],
        )(*results)

    split = P(("blk", "head"), None)
    return jax.shard_map(
        per_device,
        mesh=mesh,
        in_specs=(split, split, split, split, P()),
        out_specs=(split, split, split, split),
        check_vma=False,
    )
```

```python
import functools
import math

import jax
import jax.numpy as jnp
from jax import lax
from jax.experimental import pallas as pl
from jax.experimental.pallas import tpu as pltpu
from jax.sharding import PartitionSpec as P

HEAD_DIM = 128
EXCLUDED = -1e30
MESH = pl.DeviceIdType.MESH


def kernel(
    back, total, lens, q_hbm, k_hbm, v_hbm, do_hbm, attbuf, dqbuf, dkbuf, dvbuf,
    window, qbuf, dobuf, part, landed, own, bias,
    kv_in, q_in, kv_send, kv_recv, g_send, g_recv,
):
    rows = q_hbm.shape[0]
    kv_heads = k_hbm.shape[1] // HEAD_DIM
    groups = q_hbm.shape[1] // k_hbm.shape[1]
    width = groups * HEAD_DIM
    span = (back + 1) * rows
    scaling = HEAD_DIM ** (-0.5)
    me = lax.axis_index("blk") * back + lax.axis_index("head")

    def device(number):
        return {"blk": number // back, "head": number % back}

    def columns(g, size):
        return pl.ds(pl.multiple_of(g * size, size), size)

    def slot(k):
        return pl.ds((back - k) * rows, rows)

    def kv_load(g, which):
        return pltpu.make_async_copy(
            (k_hbm, v_hbm)[which].at[:, columns(g, HEAD_DIM)],
            window.at[g, which, slot(0), :],
            kv_in.at[which, g],
        )

    def q_load(g, which):
        return pltpu.make_async_copy(
            (q_hbm, do_hbm)[which].at[:, columns(g, width)],
            (qbuf, dobuf)[which].at[g],
            q_in.at[which, g],
        )

    def kv_copy(g, k):
        return pltpu.make_async_remote_copy(
            src_ref=window.at[g, :, slot(0), :],
            dst_ref=window.at[g, :, slot(k), :],
            send_sem=kv_send.at[k - 1, g],
            recv_sem=kv_recv.at[k - 1, g],
            device_id=device(me + k),
            device_id_type=MESH,
        )

    def g_copy(g, k):
        return pltpu.make_async_remote_copy(
            src_ref=part.at[g, :, slot(k), :],
            dst_ref=landed.at[g, k - 1],
            send_sem=g_send.at[k - 1, g],
            recv_sem=g_recv.at[k - 1, g],
            device_id=device(me - k),
            device_id_type=MESH,
        )

    @pl.loop(0, kv_heads)
    def _(g):
        kv_load(g, 0).start()
        kv_load(g, 1).start()

    barrier = pltpu.get_barrier_semaphore()
    for k in range(1, back + 1):
        @pl.when(me - k >= 0)
        def _():
            pl.semaphore_signal(barrier, inc=1, device_id=device(me - k), device_id_type=MESH)

    @pl.loop(0, kv_heads)
    def _(g):
        q_load(g, 0).start()
        q_load(g, 1).start()

    @pl.when(me < total - 1)
    def _():
        pl.semaphore_wait(barrier, jnp.minimum(total - 1 - me, back))

    @pl.loop(0, kv_heads)
    def _(g):
        kv_load(g, 0).wait()
        kv_load(g, 1).wait()
        for k in range(1, back + 1):
            @pl.when(me + k < total)
            def _():
                kv_copy(g, k).start()

    for k in range(1, back + 1):
        @pl.when(me - k < 0)
        def _():
            window[:, :, slot(k), :] = jnp.zeros((kv_heads, 2, rows, HEAD_DIM), jnp.bfloat16)

        @pl.when(me + k >= total)
        def _():
            landed[:, k - 1] = jnp.zeros((kv_heads, 2, rows, HEAD_DIM), jnp.bfloat16)

    query_pos = me * rows + lax.broadcasted_iota(jnp.int32, (1, rows), 1)

    def latest(d, carry):
        start, first = carry
        return start + lens[d], jnp.where(query_pos >= start, start, first)

    _, first = lax.fori_loop(
        0, lens.shape[0], latest, (jnp.int32(0), jnp.zeros((1, rows), jnp.int32))
    )
    key_pos = (me - back) * rows + lax.broadcasted_iota(jnp.int32, (span, rows), 0)
    bias[...] = jnp.where((key_pos <= query_pos) & (key_pos >= first), 0.0, EXCLUDED)

    def dot(a, b, a_dim, b_dim):
        return lax.dot_general(
            a, b, (((a_dim,), (b_dim,)), ((), ())), preferred_element_type=jnp.float32
        )

    def stacked(values):
        return jnp.concatenate(
            [values[:, h * HEAD_DIM : (h + 1) * HEAD_DIM] for h in range(groups)], axis=0
        )

    @pl.loop(0, kv_heads)
    def _(g):
        q_load(g, 0).wait()
        q_load(g, 1).wait()
        for k in range(1, back + 1):
            @pl.when(me - k >= 0)
            def _():
                kv_copy(g, k).wait_recv()

        keys, values = window[g, 0], window[g, 1]
        queries, grads = stacked(qbuf[g]), stacked(dobuf[g])
        kept = jnp.concatenate([bias[...]] * groups, axis=1)
        scores = dot(keys, queries, 1, 1) * (scaling * math.log2(math.e)) + kept
        peak = jnp.max(scores, axis=0, keepdims=True)
        raised = jnp.exp2(scores - peak)
        weights = raised * (1.0 / jnp.sum(raised, axis=0, keepdims=True))
        weights_bf = weights.astype(jnp.bfloat16)
        attended = dot(values, weights_bf, 0, 0)
        grad_weights = dot(values, grads, 1, 1)
        delta = jnp.sum(weights * grad_weights, axis=0, keepdims=True)
        grad_scores = (weights * (grad_weights - delta)).astype(jnp.bfloat16)
        grad_query = dot(keys, grad_scores, 0, 0) * scaling
        grad_key = dot(grad_scores, queries, 1, 0) * scaling
        grad_value = dot(weights_bf, grads, 1, 0)
        part[g, 0] = grad_key[: back * rows].astype(jnp.bfloat16)
        part[g, 1] = grad_value[: back * rows].astype(jnp.bfloat16)
        own[g, 0] = grad_key[back * rows :]
        own[g, 1] = grad_value[back * rows :]
        for h in range(groups):
            at = slice(h * HEAD_DIM, (h + 1) * HEAD_DIM)
            to = columns(g * groups + h, HEAD_DIM)
            attbuf[:, to] = attended[:, at].T.astype(jnp.bfloat16)
            dqbuf[:, to] = grad_query[:, at].T.astype(jnp.bfloat16)
        for k in range(1, back + 1):
            @pl.when(me - k >= 0)
            def _():
                g_copy(g, k).start()

    @pl.loop(0, kv_heads)
    def _(g):
        for k in range(1, back + 1):
            @pl.when(me + k < total)
            def _():
                g_copy(g, k).wait_recv()
        sums = own[g]
        for k in range(1, back + 1):
            sums = sums + landed[g, k - 1].astype(jnp.float32)
        dkbuf[:, columns(g, HEAD_DIM)] = sums[0].astype(jnp.bfloat16)
        dvbuf[:, columns(g, HEAD_DIM)] = sums[1].astype(jnp.bfloat16)

    @pl.loop(0, kv_heads)
    def _(g):
        for k in range(1, back + 1):
            @pl.when(me + k < total)
            def _():
                kv_copy(g, k).wait_send()

            @pl.when(me - k >= 0)
            def _():
                g_copy(g, k).wait_send()


def write_out(att, dq, dk, dv, att_hbm, dq_hbm, dk_hbm, dv_hbm, sems):
    copies = []
    pairs = ((att, att_hbm), (dq, dq_hbm), (dk, dk_hbm), (dv, dv_hbm))
    for which, (source, target) in enumerate(pairs):
        step = source.shape[0] // sems.shape[1]
        for piece in range(sems.shape[1]):
            at = slice(piece * step, (piece + 1) * step)
            copies.append(
                pltpu.make_async_copy(source.at[at], target.at[at], sems.at[which, piece])
            )
    for copy in copies:
        copy.start()
    for copy in copies:
        copy.wait()


def solution(mesh):
    back = mesh.shape["head"]
    total = mesh.shape["blk"] * back

    def per_device(query, key, value, grad_out, doc_lengths):
        rows, kv_heads = query.shape[0], key.shape[1] // HEAD_DIM
        width = query.shape[1] // kv_heads
        bf, f32 = jnp.bfloat16, jnp.float32
        anywhere = pl.BlockSpec(memory_space=pl.ANY)
        dma = pltpu.SemaphoreType.DMA
        results = pl.pallas_call(
            functools.partial(kernel, back, total),
            out_shape=[
                pltpu.VMEM(query.shape, bf),
                pltpu.VMEM(query.shape, bf),
                pltpu.VMEM(key.shape, bf),
                pltpu.VMEM(key.shape, bf),
            ],
            in_specs=[pl.BlockSpec(memory_space=pltpu.SMEM)] + [anywhere] * 4,
            out_specs=[pl.BlockSpec(memory_space=pltpu.VMEM)] * 4,
            scratch_shapes=[
                pltpu.VMEM((kv_heads, 2, (back + 1) * rows, HEAD_DIM), bf),
                pltpu.VMEM((kv_heads, rows, width), bf),
                pltpu.VMEM((kv_heads, rows, width), bf),
                pltpu.VMEM((kv_heads, 2, back * rows, HEAD_DIM), bf),
                pltpu.VMEM((kv_heads, back, 2, rows, HEAD_DIM), bf),
                pltpu.VMEM((kv_heads, 2, rows, HEAD_DIM), f32),
                pltpu.VMEM(((back + 1) * rows, rows), f32),
                dma((2, kv_heads)),
                dma((2, kv_heads)),
                dma((back, kv_heads)),
                dma((back, kv_heads)),
                dma((back, kv_heads)),
                dma((back, kv_heads)),
            ],
            compiler_params=pltpu.CompilerParams(collective_id=0, has_side_effects=True),
        )(doc_lengths, query, key, value, grad_out)
        results = [pltpu.with_memory_space_constraint(r, pltpu.VMEM) for r in results]
        return pl.pallas_call(
            write_out,
            out_shape=[
                jax.ShapeDtypeStruct(query.shape, bf),
                jax.ShapeDtypeStruct(query.shape, bf),
                jax.ShapeDtypeStruct(key.shape, bf),
                jax.ShapeDtypeStruct(key.shape, bf),
            ],
            in_specs=[pl.BlockSpec(memory_space=pltpu.VMEM)] * 4,
            out_specs=[anywhere] * 4,
            scratch_shapes=[dma((4, 4))],
        )(*results)

    split = P(("blk", "head"), None)
    return jax.shard_map(
        per_device,
        mesh=mesh,
        in_specs=(split, split, split, split, P()),
        out_specs=(split, split, split, split),
        check_vma=False,
    )
```

```python
import functools
import math

import jax
import jax.numpy as jnp
from jax import lax
from jax.experimental import pallas as pl
from jax.experimental.pallas import tpu as pltpu
from jax.sharding import PartitionSpec as P

HEAD_DIM = 128
EXCLUDED = -1e30
MESH = pl.DeviceIdType.MESH


def kernel(
    back, total, lens, q_hbm, k_hbm, v_hbm, do_hbm, attbuf, dqbuf, dkbuf, dvbuf,
    window, qbuf, dobuf, part, landed, own, bias,
    kv_in, q_in, kv_send, kv_recv, g_send, g_recv,
):
    rows = q_hbm.shape[0]
    kv_heads = k_hbm.shape[1] // HEAD_DIM
    groups = q_hbm.shape[1] // k_hbm.shape[1]
    width = groups * HEAD_DIM
    span = (back + 1) * rows
    scaling = HEAD_DIM ** (-0.5)
    me = lax.axis_index("blk") * back + lax.axis_index("head")

    def device(number):
        return {"blk": number // back, "head": number % back}

    def columns(g, size):
        return pl.ds(pl.multiple_of(g * size, size), size)

    def slot(k):
        return pl.ds((back - k) * rows, rows)

    def kv_load(g, which):
        return pltpu.make_async_copy(
            (k_hbm, v_hbm)[which].at[:, columns(g, HEAD_DIM)],
            window.at[g, which, slot(0), :],
            kv_in.at[which, g],
        )

    def q_load(g, which):
        return pltpu.make_async_copy(
            (q_hbm, do_hbm)[which].at[:, columns(g, width)],
            (qbuf, dobuf)[which].at[g],
            q_in.at[which, g],
        )

    def kv_copy(g, k):
        return pltpu.make_async_remote_copy(
            src_ref=window.at[g, :, slot(0), :],
            dst_ref=window.at[g, :, slot(k), :],
            send_sem=kv_send.at[k - 1, g],
            recv_sem=kv_recv.at[k - 1, g],
            device_id=device(me + k),
            device_id_type=MESH,
        )

    def g_copy(g, k):
        return pltpu.make_async_remote_copy(
            src_ref=part.at[g, :, slot(k), :],
            dst_ref=landed.at[g, k - 1],
            send_sem=g_send.at[k - 1, g],
            recv_sem=g_recv.at[k - 1, g],
            device_id=device(me - k),
            device_id_type=MESH,
        )

    @pl.loop(0, kv_heads)
    def _(g):
        kv_load(g, 0).start()
        kv_load(g, 1).start()

    barrier = pltpu.get_barrier_semaphore()
    for k in range(1, back + 1):
        @pl.when(me - k >= 0)
        def _():
            pl.semaphore_signal(barrier, inc=1, device_id=device(me - k), device_id_type=MESH)

    @pl.when(me < total - 1)
    def _():
        pl.semaphore_wait(barrier, jnp.minimum(total - 1 - me, back))

    @pl.loop(0, kv_heads)
    def _(g):
        kv_load(g, 0).wait()
        kv_load(g, 1).wait()
        for k in range(1, back + 1):
            @pl.when(me + k < total)
            def _():
                kv_copy(g, k).start()

    @pl.loop(0, kv_heads)
    def _(g):
        q_load(g, 0).start()
        q_load(g, 1).start()

    for k in range(1, back + 1):
        @pl.when(me - k < 0)
        def _():
            window[:, :, slot(k), :] = jnp.zeros((kv_heads, 2, rows, HEAD_DIM), jnp.bfloat16)

        @pl.when(me + k >= total)
        def _():
            landed[:, k - 1] = jnp.zeros((kv_heads, 2, rows, HEAD_DIM), jnp.bfloat16)

    query_pos = me * rows + lax.broadcasted_iota(jnp.int32, (1, rows), 1)

    def latest(d, carry):
        start, first = carry
        return start + lens[d], jnp.where(query_pos >= start, start, first)

    _, first = lax.fori_loop(
        0, lens.shape[0], latest, (jnp.int32(0), jnp.zeros((1, rows), jnp.int32))
    )
    key_pos = (me - back) * rows + lax.broadcasted_iota(jnp.int32, (span, rows), 0)
    bias[...] = jnp.where((key_pos <= query_pos) & (key_pos >= first), 0.0, EXCLUDED)

    def dot(a, b, a_dim, b_dim):
        return lax.dot_general(
            a, b, (((a_dim,), (b_dim,)), ((), ())), preferred_element_type=jnp.float32
        )

    def stacked(values):
        return jnp.concatenate(
            [values[:, h * HEAD_DIM : (h + 1) * HEAD_DIM] for h in range(groups)], axis=0
        )

    @pl.loop(0, kv_heads)
    def _(g):
        q_load(g, 0).wait()
        q_load(g, 1).wait()
        for k in range(1, back + 1):
            @pl.when(me - k >= 0)
            def _():
                kv_copy(g, k).wait_recv()

        keys, values = window[g, 0], window[g, 1]
        queries, grads = stacked(qbuf[g]), stacked(dobuf[g])
        kept = jnp.concatenate([bias[...]] * groups, axis=1)
        scores = dot(keys, queries, 1, 1) * (scaling * math.log2(math.e)) + kept
        peak = jnp.max(scores, axis=0, keepdims=True)
        raised = jnp.exp2(scores - peak)
        weights = raised * (1.0 / jnp.sum(raised, axis=0, keepdims=True))
        weights_bf = weights.astype(jnp.bfloat16)
        attended = dot(values, weights_bf, 0, 0)
        grad_weights = dot(values, grads, 1, 1)
        delta = jnp.sum(weights * grad_weights, axis=0, keepdims=True)
        grad_scores = (weights * (grad_weights - delta)).astype(jnp.bfloat16)
        grad_query = dot(keys, grad_scores, 0, 0) * scaling
        grad_key = dot(grad_scores, queries, 1, 0) * scaling
        grad_value = dot(weights_bf, grads, 1, 0)
        part[g, 0] = grad_key[: back * rows].astype(jnp.bfloat16)
        part[g, 1] = grad_value[: back * rows].astype(jnp.bfloat16)
        own[g, 0] = grad_key[back * rows :]
        own[g, 1] = grad_value[back * rows :]
        for h in range(groups):
            at = slice(h * HEAD_DIM, (h + 1) * HEAD_DIM)
            to = columns(g * groups + h, HEAD_DIM)
            attbuf[:, to] = attended[:, at].T.astype(jnp.bfloat16)
            dqbuf[:, to] = grad_query[:, at].T.astype(jnp.bfloat16)
        for k in range(1, back + 1):
            @pl.when(me - k >= 0)
            def _():
                g_copy(g, k).start()

    @pl.loop(0, kv_heads)
    def _(g):
        for k in range(1, back + 1):
            @pl.when(me + k < total)
            def _():
                g_copy(g, k).wait_recv()
        sums = own[g]
        for k in range(1, back + 1):
            sums = sums + landed[g, k - 1].astype(jnp.float32)
        dkbuf[:, columns(g, HEAD_DIM)] = sums[0].astype(jnp.bfloat16)
        dvbuf[:, columns(g, HEAD_DIM)] = sums[1].astype(jnp.bfloat16)

    @pl.loop(0, kv_heads)
    def _(g):
        for k in range(1, back + 1):
            @pl.when(me + k < total)
            def _():
                kv_copy(g, k).wait_send()

            @pl.when(me - k >= 0)
            def _():
                g_copy(g, k).wait_send()


def write_out(att, dq, dk, dv, att_hbm, dq_hbm, dk_hbm, dv_hbm, sems):
    copies = []
    pairs = ((att, att_hbm), (dq, dq_hbm), (dk, dk_hbm), (dv, dv_hbm))
    for which, (source, target) in enumerate(pairs):
        step = source.shape[0] // sems.shape[1]
        for piece in range(sems.shape[1]):
            at = slice(piece * step, (piece + 1) * step)
            copies.append(
                pltpu.make_async_copy(source.at[at], target.at[at], sems.at[which, piece])
            )
    for copy in copies:
        copy.start()
    for copy in copies:
        copy.wait()


def solution(mesh):
    back = mesh.shape["head"]
    total = mesh.shape["blk"] * back

    def per_device(query, key, value, grad_out, doc_lengths):
        rows, kv_heads = query.shape[0], key.shape[1] // HEAD_DIM
        width = query.shape[1] // kv_heads
        bf, f32 = jnp.bfloat16, jnp.float32
        anywhere = pl.BlockSpec(memory_space=pl.ANY)
        dma = pltpu.SemaphoreType.DMA
        results = pl.pallas_call(
            functools.partial(kernel, back, total),
            out_shape=[
                pltpu.VMEM(query.shape, bf),
                pltpu.VMEM(query.shape, bf),
                pltpu.VMEM(key.shape, bf),
                pltpu.VMEM(key.shape, bf),
            ],
            in_specs=[pl.BlockSpec(memory_space=pltpu.SMEM)] + [anywhere] * 4,
            out_specs=[pl.BlockSpec(memory_space=pltpu.VMEM)] * 4,
            scratch_shapes=[
                pltpu.VMEM((kv_heads, 2, (back + 1) * rows, HEAD_DIM), bf),
                pltpu.VMEM((kv_heads, rows, width), bf),
                pltpu.VMEM((kv_heads, rows, width), bf),
                pltpu.VMEM((kv_heads, 2, back * rows, HEAD_DIM), bf),
                pltpu.VMEM((kv_heads, back, 2, rows, HEAD_DIM), bf),
                pltpu.VMEM((kv_heads, 2, rows, HEAD_DIM), f32),
                pltpu.VMEM(((back + 1) * rows, rows), f32),
                dma((2, kv_heads)),
                dma((2, kv_heads)),
                dma((back, kv_heads)),
                dma((back, kv_heads)),
                dma((back, kv_heads)),
                dma((back, kv_heads)),
            ],
            compiler_params=pltpu.CompilerParams(collective_id=0, has_side_effects=True),
        )(doc_lengths, query, key, value, grad_out)
        results = [pltpu.with_memory_space_constraint(r, pltpu.VMEM) for r in results]
        return pl.pallas_call(
            write_out,
            out_shape=[
                jax.ShapeDtypeStruct(query.shape, bf),
                jax.ShapeDtypeStruct(query.shape, bf),
                jax.ShapeDtypeStruct(key.shape, bf),
                jax.ShapeDtypeStruct(key.shape, bf),
            ],
            in_specs=[pl.BlockSpec(memory_space=pltpu.VMEM)] * 4,
            out_specs=[anywhere] * 4,
            scratch_shapes=[dma((4, 4))],
        )(*results)

    split = P(("blk", "head"), None)
    return jax.shard_map(
        per_device,
        mesh=mesh,
        in_specs=(split, split, split, split, P()),
        out_specs=(split, split, split, split),
        check_vma=False,
    )
```
